1024 devices in a mesh: fsdp: 64 (over x_hi, z), dp: 16 (over x_lo, y, core).
Axes of the slice: x: 4 (x_hi: 2, x_lo: 2; x = x_hi * 2 + x_lo), y: 4, z: 32, core: 2. Of those that a mesh axis runs over, the one named last changes fastest.
Arguments:
- qkv: bfloat16 [262144, 768], P(('fsdp', 'dp')), may hold values from -6 to 6
- segment: int32 [1024, 256], P(('fsdp', 'dp')), may hold values from 0 to 3, as said below
- handoff: int32 [1024], P(('fsdp', 'dp')), may hold values from 0 to 3, as said below
- qk_gain: float32 [2, 256], replicated, may hold values from 0.6 to 6
- d_head: bfloat16 [262144, 256], P(('fsdp', 'dp')), may hold values from -12 to 12
Outputs:
- grad_qkv: bfloat16 [262144, 768], P(('fsdp', 'dp'))
- attended: bfloat16 [262144, 256], P(('fsdp', 'dp'))
- handed: bfloat16 [1024, 160, 256], P(('fsdp', 'dp'))
- grad_gain: float32 [2, 256], replicated
The draws below stay inside these ranges and needn't reach their ends.
Inputs may be any that keep to these rules, and one draw needn't show every extreme that they name: `segment`: image ids never fall along a pack; each of the 4 images of a pack has 1 to 160 patches, and one image of every pack has exactly 160. `handoff`: names an image of its own pack.
All inputs are finite; a program needn't handle non-finite values.
Results may differ from the reference program's by a relative error of at most 0.006.
The reference program's roundings to bfloat16 on the way count: a program that leaves them out, or rounds other values in their place, can miss the bound.
Values may be sent and summed in bfloat16 or wider, within the bound.
A program may use at most 32 MiB of HBM per device.

```python
import jax
import jax.numpy as jnp
from jax import lax

HEAD = 128
HEADS = 2
TOK_DEV = 256
IMAGES = 4
MOST = 160
PACKS = 1024
TOKENS = 262144


def pack_layout(key):
    base_key = jax.random.fold_in(key, 7001)
    key_split = jax.random.split(base_key, PACKS)

    def one_pack(pack_key):
        key_a, key_b, key_c, key_d, key_e = jax.random.split(pack_key, 5)
        remaining = TOK_DEV - MOST
        first_len = jax.random.randint(key_a, (), 1, remaining - 1)
        second_len = jax.random.randint(key_b, (), 1, remaining - first_len)
        third_len = remaining - first_len - second_len
        long_spot = jax.random.randint(key_c, (), 0, IMAGES)
        others = jnp.stack([first_len, second_len, third_len])
        image_index = jnp.arange(IMAGES, dtype=jnp.int32)
        other_index = jnp.clip(image_index - (image_index > long_spot).astype(jnp.int32), 0, 2)
        lengths = jnp.where(image_index == long_spot, MOST, others[other_index]).astype(jnp.int32)
        image_ends = jnp.cumsum(lengths)
        positions = jnp.arange(TOK_DEV, dtype=jnp.int32)
        seg_ids = jnp.sum((positions[:, None] >= image_ends[None, :]).astype(jnp.int32), axis=1)
        coin_flip = jax.random.randint(key_d, (), 0, 2)
        other_pick = jax.random.randint(key_e, (), 0, IMAGES)
        handed_pick = jnp.where(coin_flip == 1, long_spot, other_pick)
        return (seg_ids.astype(jnp.int32), handed_pick.astype(jnp.int32), long_spot.astype(jnp.int32))
    seg_all, picks, spots = jax.vmap(one_pack)(key_split)
    pack_index = jnp.arange(PACKS, dtype=jnp.int32)
    picks = jnp.where(pack_index == 0, spots, picks)
    return (seg_all, picks)


def draw_segment(key, part):
    return pack_layout(key)[0]


def draw_handoff(key, part):
    return pack_layout(key)[1]


def draw_qk_gain(key, part):
    return jnp.exp(jax.random.uniform(key, (2, HEADS * HEAD), jnp.float32, -0.5, 0.5))


def draw_d_head(key, part):
    rising = 1.0 + 2.0 * jnp.arange(PACKS, dtype=jnp.float32) / max(PACKS - 1, 1)
    row_scale = jnp.repeat(rising, TOK_DEV)[:, None]
    values = jax.random.truncated_normal(key, -4.0, 4.0, (TOKENS, HEADS * HEAD), jnp.float32)
    return (values * row_scale).astype(jnp.bfloat16)


def block_levels(own_key, extent, shards, smallest, high):
    loudness = 1.0
    for axis_at, shards_of in shards:
        steps = jax.random.uniform(jax.random.fold_in(jax.random.fold_in(own_key, 6), axis_at), (shards_of,), jnp.float32, smallest / len(shards), high / len(shards))
        loudness = loudness * jnp.repeat(jnp.exp(steps), extent[axis_at] // shards_of).reshape((-1,) + (1,) * (len(extent) - 1 - axis_at))
    return loudness


def normal_values(stream_key, shape, scale, limit, cuts=(), held_as=jnp.bfloat16):
    result = scale * jax.random.normal(stream_key, shape, jnp.float32)
    if cuts:
        result = result * block_levels(stream_key, shape, cuts, -0.22, 0.18)
    return jnp.clip(result, -limit, limit).astype(held_as)


def setup_inputs(seed: int = 0) -> dict:
    keys = jax.random.split(jax.random.key(seed), 6)
    qkv = normal_values(keys[0], (TOKENS, 3 * HEADS * HEAD), 1.0, 6.0, ((0, 1024),))
    segment = draw_segment(jax.random.fold_in(keys[5], 71), 0)
    handoff = draw_handoff(jax.random.fold_in(keys[5], 71), 0)
    qk_gain = draw_qk_gain(jax.random.fold_in(keys[5], 71), 0)
    d_head = draw_d_head(jax.random.fold_in(keys[5], 71), 0)
    return dict(qkv=qkv, segment=segment, handoff=handoff, qk_gain=qk_gain, d_head=d_head)


epsilon = 1e-06

def head_norm(values, gain_vec):
    centre = lax.optimization_barrier(jnp.mean(values, axis=-1, keepdims=True))
    shifted = values - centre
    spread = lax.optimization_barrier(jnp.mean(shifted * shifted, axis=-1, keepdims=True))
    inverse = lax.rsqrt(spread + epsilon)
    centred = shifted * inverse
    return (centred * gain_vec, centred, inverse)

def norm_back(grad_out, centred, inverse, gain_vec):
    scaled = grad_out * gain_vec
    mean_first = lax.optimization_barrier(jnp.mean(scaled, axis=-1, keepdims=True))
    mean_second = lax.optimization_barrier(jnp.mean(scaled * centred, axis=-1, keepdims=True))
    return inverse * (scaled - mean_first - centred * mean_second)

def attend_heads(qkv_rows, allowed, cotangent, qk_gain):
    head_width = cotangent.shape[1]
    head_count = head_width // HEAD
    scaling = 1.0 / jnp.sqrt(jnp.float32(HEAD))
    outputs = []
    query_grads = []
    key_grads = []
    value_grads = []
    query_terms = []
    key_terms = []
    for head_index in range(head_count):
        col_low = head_index * HEAD
        col_high = col_low + HEAD
        query_part = qkv_rows[:, col_low:col_high].astype(jnp.float32)
        key_part = qkv_rows[:, head_width + col_low:head_width + col_high].astype(jnp.float32)
        value_low = qkv_rows[:, 2 * head_width + col_low:2 * head_width + col_high]
        d_rows = cotangent[:, col_low:col_high]
        gain_query = qk_gain[0, col_low:col_high]
        gain_keys = qk_gain[1, col_low:col_high]
        query_n, query_hat, query_inv = head_norm(query_part, gain_query)
        keys_n, keys_hat, keys_inv = head_norm(key_part, gain_keys)
        query_low = query_n.astype(jnp.bfloat16)
        keys_low = keys_n.astype(jnp.bfloat16)
        scores = jnp.dot(query_low, keys_low.T, preferred_element_type=jnp.float32) * scaling
        scores = jnp.where(allowed, scores, jnp.float32(-1e+30))
        scores = scores - lax.optimization_barrier(jnp.max(scores, axis=-1, keepdims=True))
        exp_scores = jnp.where(allowed, jnp.exp(scores), jnp.float32(0.0))
        attend = exp_scores / lax.optimization_barrier(jnp.sum(exp_scores, axis=-1, keepdims=True))
        attend_low = attend.astype(jnp.bfloat16)
        outputs.append(jnp.dot(attend_low, value_low, preferred_element_type=jnp.float32).astype(jnp.bfloat16))
        grad_attend = jnp.dot(d_rows, value_low.T, preferred_element_type=jnp.float32)
        inner_sum = lax.optimization_barrier(jnp.sum(grad_attend * attend, axis=-1, keepdims=True))
        grad_scores = (attend * (grad_attend - inner_sum) * scaling).astype(jnp.bfloat16)
        grad_query = jnp.dot(grad_scores, keys_low, preferred_element_type=jnp.float32)
        grad_keys = jnp.dot(grad_scores.T, query_low, preferred_element_type=jnp.float32)
        grad_value = jnp.dot(attend_low.T, d_rows, preferred_element_type=jnp.float32)
        query_terms.append(lax.optimization_barrier(jnp.sum(grad_query * query_hat, axis=0)))
        key_terms.append(lax.optimization_barrier(jnp.sum(grad_keys * keys_hat, axis=0)))
        query_grads.append(norm_back(grad_query, query_hat, query_inv, gain_query))
        key_grads.append(norm_back(grad_keys, keys_hat, keys_inv, gain_keys))
        value_grads.append(grad_value)
    output = jnp.concatenate(outputs, axis=1)
    grads = jnp.concatenate(query_grads + key_grads + value_grads, axis=1).astype(jnp.bfloat16)
    gain_terms = jnp.stack([jnp.concatenate(query_terms), jnp.concatenate(key_terms)])
    return (output, grads, gain_terms)

def reference(qkv, segment, handoff, qk_gain, d_head):
    pack_count = segment.shape[0]
    pack_rows = segment.shape[1]
    blocks = qkv.reshape(pack_count, pack_rows, qkv.shape[1])
    cotangents = d_head.reshape(pack_count, pack_rows, d_head.shape[1])

    def one_pack(gain_sum, items):
        block, seg_row, d_rows = items
        allowed = seg_row[:, None] == seg_row[None, :]
        output, grads, gain_terms = attend_heads(block, allowed, d_rows, qk_gain)
        return (gain_sum + gain_terms, (output, grads))
    start_sum = jnp.zeros((2, d_head.shape[1]), jnp.float32)
    grad_gain, (outputs, grads) = lax.scan(one_pack, start_sum, (blocks, segment, cotangents))
    handed_rows = segment == handoff[:, None]
    attended = jnp.where(handed_rows[:, :, None], jnp.zeros_like(outputs), outputs)
    first_row = lax.optimization_barrier(jnp.sum((segment < handoff[:, None]).astype(jnp.int32), axis=1))
    image_len = lax.optimization_barrier(jnp.sum(handed_rows.astype(jnp.int32), axis=1))
    slot_index = jnp.arange(MOST, dtype=jnp.int32)
    row_index = jnp.minimum(first_row[:, None] + slot_index[None, :], pack_rows - 1).astype(jnp.int32)
    taken = jnp.take_along_axis(outputs, row_index[:, :, None], axis=1)
    in_image = (slot_index[None, :] < image_len[:, None])[:, :, None]
    taken = jnp.where(in_image, taken, jnp.zeros_like(taken))
    pack_index = jnp.arange(pack_count, dtype=jnp.int32)
    partner = (pack_index + 1 - 2 * (pack_index % 2)).astype(jnp.int32)
    handed = taken[partner]
    return (grads.reshape(qkv.shape), attended.reshape(d_head.shape), handed, grad_gain)
```

```python
import jax
import jax.numpy as jnp
from jax import lax
from jax.experimental import pallas as pl
from jax.experimental.pallas import tpu as pltpu
from jax.sharding import Mesh
from jax.sharding import PartitionSpec as P

HEAD = 128
HEADS = 2
ROWS = 256
WIDTH = HEADS * HEAD
MOST = 160
IMAGES = 4
EPSILON = 1e-06
SCALE = 1.0 / HEAD**0.5

AXES = ("fsdp_0", "fsdp_1", "dp_0", "dp_1", "dp_2")
PLANES = 32
PLANE = 32
QUAD = 4
GROUPS = PLANES // QUAD
NEAR = sorted(((i, j) for i in range(4) for j in range(4)), key=lambda o: -(min(o[0], 4 - o[0]) + min(o[1], 4 - o[1])))
LOGICAL = pl.DeviceIdType.LOGICAL
F32 = jnp.float32
BF16 = jnp.bfloat16


def dot(a, b, a_dim, b_dim):
    return lax.dot_general(a, b, (((a_dim,), (b_dim,)), ((), ())), preferred_element_type=F32)


def head_norm(values, gain):
    shifted = values - jnp.mean(values, axis=-1, keepdims=True)
    inverse = lax.rsqrt(jnp.mean(shifted * shifted, axis=-1, keepdims=True) + EPSILON)
    hat = shifted * inverse
    return (hat * gain).astype(BF16), hat, inverse


def norm_back(grad, hat, inverse, gain):
    scaled = grad * gain
    first = jnp.mean(scaled, axis=-1, keepdims=True)
    second = jnp.mean(scaled * hat, axis=-1, keepdims=True)
    return inverse * (scaled - first - hat * second)


def kernel(
    qkv, seg, hand, gain, d_head,
    grad_out, attended_out, handed_out, sum_out,
    qkv_v, seg_v, hand_s, gain_v, d_v, taken_v, plane_v, quad_v, ring_v,
    load_sem, plane_send, plane_recv, quad_send, quad_recv, ring_send, ring_recv, hand_sem,
):
    x_hi, z, x_lo, y, core = (lax.axis_index(a) for a in AXES)
    low = x_lo * 8 + y * 2 + core
    mine = x_hi * 16 + low
    quad_at = lax.rem(z, QUAD)
    group_at = lax.div(z, QUAD)

    x = 2 * x_hi + x_lo
    xs = [lax.rem(x + k, 4) for k in range(4)]
    ys = [lax.rem(y + k, 4) for k in range(4)]
    cores = [core, 1 - core]
    slot_x = [8 * k for k in xs]
    device_x = [lax.div(k, 2) * 512 + lax.rem(k, 2) * 8 + z * 16 for k in xs]
    slot_y = [[2 * k + c for c in cores] for k in ys]
    plane = [
        (slot_x[i] + slot_y[j][c], device_x[i] + slot_y[j][c])
        for i, j in NEAR for c in range(2) if (i, j, c) != (0, 0, 0)
    ]

    def z_device(other):
        return x_hi * 512 + other * 16 + low

    partner = x_hi * 512 + z * 16 + low + 1 - 2 * core
    quad_at_of = [lax.rem(quad_at + k, QUAD) for k in range(QUAD)]
    quads = [group_at * QUAD + quad_at_of[k] for k in range(QUAD)]

    def at_offset(offset):
        return lax.rem(z + (offset + PLANES), PLANES)

    loads = [
        pltpu.make_async_copy(a, b, load_sem.at[i])
        for i, (a, b) in enumerate(((qkv, qkv_v), (seg, seg_v), (gain, gain_v), (d_head, d_v), (hand, hand_s)))
    ]
    for load in loads:
        load.start()
    barrier = pltpu.get_barrier_semaphore()

    for _, device in plane:
        pl.semaphore_signal(barrier, inc=1, device_id=device, device_id_type=LOGICAL)
    far = [quads[k] for k in range(1, QUAD)] + [at_offset(o) for o in (4, -4, 8, -8)]
    for other in far:
        pl.semaphore_signal(barrier, inc=1, device_id=z_device(other), device_id_type=LOGICAL)
    for load in loads:
        load.wait()

    seg_row = seg_v[...].astype(F32)
    row_id = lax.broadcasted_iota(jnp.int32, (ROWS, 1), 0).astype(F32)
    seg_col = jnp.zeros((ROWS, 1), F32)
    for image in range(1, IMAGES):
        end = jnp.sum(jnp.where(seg_row < image, 1.0, 0.0), axis=1, keepdims=True)
        seg_col = seg_col + jnp.where(row_id >= end, 1.0, 0.0)
    allowed = seg_col == seg_row
    gains = gain_v[...]
    kept = []
    terms = [[], []]
    for head in range(HEADS):
        cols = pl.ds(head * HEAD, HEAD)
        gain_q = gains[0:1, head * HEAD:(head + 1) * HEAD]
        gain_k = gains[1:2, head * HEAD:(head + 1) * HEAD]
        query_b, query_hat, query_inv = head_norm(qkv_v[:, cols].astype(F32), gain_q)
        keys_b, keys_hat, keys_inv = head_norm(qkv_v[:, pl.ds(WIDTH + head * HEAD, HEAD)].astype(F32), gain_k)
        value_b = qkv_v[:, pl.ds(2 * WIDTH + head * HEAD, HEAD)]
        d_b = d_v[:, cols]
        scores = jnp.where(allowed, dot(query_b, keys_b, 1, 1) * SCALE, -1e30)
        scores = scores - jnp.max(scores, axis=-1, keepdims=True)
        exps = jnp.where(allowed, jnp.exp(scores), 0.0)
        attend = exps / jnp.sum(exps, axis=-1, keepdims=True)
        grad_attend = dot(d_b, value_b, 1, 1)
        inner = jnp.sum(grad_attend * attend, axis=-1, keepdims=True)
        grad_scores = (attend * (grad_attend - inner) * SCALE).astype(BF16)
        grad_query = dot(grad_scores, keys_b, 1, 0)
        grad_keys = dot(grad_scores, query_b, 0, 0)
        terms[0].append(jnp.sum(grad_query * query_hat, axis=0, keepdims=True))
        terms[1].append(jnp.sum(grad_keys * keys_hat, axis=0, keepdims=True))
        kept.append((attend.astype(BF16), value_b, d_b, grad_query, query_hat, query_inv, gain_q,
                     grad_keys, keys_hat, keys_inv, gain_k))
    plane_v[mine] = jnp.concatenate(terms[0] + terms[1], axis=0)

    pl.semaphore_wait(barrier, PLANE - 1 + len(far))

    plane_sends = [
        pltpu.make_async_remote_copy(
            src_ref=plane_v.at[mine], dst_ref=plane_v.at[mine], send_sem=plane_send.at[i],
            recv_sem=plane_recv.at[mine], device_id=device, device_id_type=LOGICAL)
        for i, (_, device) in enumerate(plane)
    ]
    for copy in plane_sends:
        copy.start()

    chosen = hand_s[0].astype(F32)
    is_chosen = seg_row == chosen
    first = jnp.sum(jnp.where(seg_row < chosen, 1.0, 0.0), axis=1, keepdims=True)
    col_id = lax.broadcasted_iota(jnp.int32, (MOST, ROWS), 1).astype(F32)
    slot_id = lax.broadcasted_iota(jnp.int32, (MOST, ROWS), 0).astype(F32)
    take = jnp.where(jnp.logical_and(col_id - slot_id == first, is_chosen), 1.0, 0.0).astype(BF16)
    stays = seg_col != chosen
    for head in range(HEADS):
        cols = pl.ds(head * HEAD, HEAD)
        attend_b, value_b = kept[head][:2]
        output = dot(attend_b, value_b, 1, 0).astype(BF16)
        taken_v[:, cols] = dot(take, output, 1, 0).astype(BF16)
        attended_out[:, cols] = jnp.where(stays, output.astype(F32), 0.0).astype(BF16)
    hand_copy = pltpu.make_async_remote_copy(
        src_ref=taken_v, dst_ref=handed_out, send_sem=hand_sem.at[0], recv_sem=hand_sem.at[1],
        device_id=partner, device_id_type=LOGICAL)
    hand_copy.start()
    for head in range(HEADS):
        (attend_b, value_b, d_b, grad_query, query_hat, query_inv, gain_q,
         grad_keys, keys_hat, keys_inv, gain_k) = kept[head]
        grad_out[:, pl.ds(head * HEAD, HEAD)] = norm_back(grad_query, query_hat, query_inv, gain_q).astype(BF16)
        grad_out[:, pl.ds(WIDTH + head * HEAD, HEAD)] = norm_back(grad_keys, keys_hat, keys_inv, gain_k).astype(BF16)
        grad_out[:, pl.ds(2 * WIDTH + head * HEAD, HEAD)] = dot(attend_b, d_b, 0, 0).astype(BF16)

    for i, (slot, device) in enumerate(plane):
        pltpu.make_async_remote_copy(
            src_ref=plane_v.at[mine], dst_ref=plane_v.at[slot], send_sem=plane_send.at[i],
            recv_sem=plane_recv.at[slot], device_id=device, device_id_type=LOGICAL).wait_recv()
    quad_v[quad_at] = jnp.sum(plane_v[:PLANE], axis=0)

    def z_copy(buf, slot, send, recv, other):
        return pltpu.make_async_remote_copy(
            src_ref=buf.at[slot], dst_ref=buf.at[slot], send_sem=send, recv_sem=recv.at[slot],
            device_id=z_device(other), device_id_type=LOGICAL)

    sends = [z_copy(quad_v, quad_at, quad_send.at[k], quad_recv, quads[k]) for k in range(1, QUAD)]
    for copy in sends:
        copy.start()
    for k in range(1, QUAD):
        z_copy(quad_v, quad_at_of[k], quad_send.at[k], quad_recv, quads[k]).wait_recv()
    ring_v[group_at] = jnp.sum(quad_v[:QUAD], axis=0)

    def slot_at(offset):
        return lax.rem(group_at + (offset + GROUPS), GROUPS)

    ring = []
    for i, offset in enumerate((8, -8, 4, -4)):
        ring.append(z_copy(ring_v, group_at, ring_send.at[i], ring_recv, at_offset(offset)))
        ring[-1].start()
    for i, (heard, target) in enumerate(((1, -8), (-1, 8), (2, -8))):
        slot = slot_at(heard)
        forward = z_copy(ring_v, slot, ring_send.at[4 + i], ring_recv, at_offset(target))
        forward.wait_recv()
        forward.start()
        ring.append(forward)
    for heard in (-2, 3, -3, 4):
        z_copy(ring_v, slot_at(heard), ring_send.at[0], ring_recv, at_offset(8)).wait_recv()
    total = jnp.sum(ring_v[:GROUPS], axis=0)
    sum_out[...] = jnp.concatenate(
        [jnp.concatenate([total[2 * i:2 * i + 1], total[2 * i + 1:2 * i + 2]], axis=1) for i in range(2)], axis=0)

    for copy in plane_sends + sends + ring:
        copy.wait_send()
    hand_copy.wait()


def write_kernel(grad, attended, handed, total, grad_out, attended_out, handed_out, sum_out, sem):
    copies = [
        pltpu.make_async_copy(a, b, sem.at[i])
        for i, (a, b) in enumerate(
            ((grad, grad_out), (attended, attended_out), (handed, handed_out.at[0]), (total, sum_out)))
    ]
    for copy in copies:
        copy.start()
    for copy in copies:
        copy.wait()


def body(qkv, segment, handoff, qk_gain, d_head):
    anywhere = pl.BlockSpec(memory_space=pl.ANY)
    hbm = pl.BlockSpec(memory_space=pltpu.HBM)
    vmem = pl.BlockSpec(memory_space=pltpu.VMEM)
    dma = pltpu.SemaphoreType.DMA
    held = (
        pltpu.VMEM((ROWS, 3 * WIDTH), BF16), pltpu.VMEM((ROWS, WIDTH), BF16),
        pltpu.VMEM((MOST, WIDTH), BF16), pltpu.VMEM((2, WIDTH), F32),
    )
    results = pl.pallas_call(
        kernel,
        out_shape=held,
        in_specs=[hbm] * 5,
        out_specs=(vmem,) * 4,
        scratch_shapes=[
            pltpu.VMEM((ROWS, 3 * WIDTH), BF16), pltpu.VMEM((1, ROWS), jnp.int32), pltpu.SMEM((1,), jnp.int32),
            pltpu.VMEM((2, WIDTH), F32), pltpu.VMEM((ROWS, WIDTH), BF16), pltpu.VMEM((MOST, WIDTH), BF16),
            pltpu.VMEM((PLANE + 1, 4, HEAD), F32), pltpu.VMEM((QUAD + 1, 4, HEAD), F32), pltpu.VMEM((GROUPS + 1, 4, HEAD), F32),
            dma((5,)), dma((PLANE,)), dma((PLANE,)), dma((QUAD,)), dma((QUAD,)), dma((8,)), dma((GROUPS,)), dma((2,)),
        ],
        compiler_params=pltpu.CompilerParams(collective_id=0, has_side_effects=True),
        name="pack_backward",
    )(qkv, segment, handoff, qk_gain, d_head)
    return pl.pallas_call(
        write_kernel,
        out_shape=(
            jax.ShapeDtypeStruct((ROWS, 3 * WIDTH), BF16), jax.ShapeDtypeStruct((ROWS, WIDTH), BF16),
            jax.ShapeDtypeStruct((1, MOST, WIDTH), BF16), jax.ShapeDtypeStruct((2, WIDTH), F32),
        ),
        in_specs=[vmem] * 4,
        out_specs=(anywhere,) * 4,
        scratch_shapes=[dma((4,))],
        name="write_out",
    )(*(pltpu.with_memory_space_constraint(r, pltpu.VMEM) for r in results))


def solution(mesh):
    split = Mesh(mesh.devices.reshape(2, 32, 2, 4, 2), AXES)
    rows = P(AXES, None)
    return jax.shard_map(
        body,
        mesh=split,
        in_specs=(rows, rows, P(AXES), P(), rows),
        out_specs=(rows, rows, P(AXES, None, None), P()),
        check_vma=False,
    )
```
